32 devices in a mesh: dp: 1 (over z), tp: 32 (over y, x, core).
Axes of the slice: x: 4, y: 4, z: 1, core: 2. Of those that a mesh axis runs over, the one named last changes fastest.
The devices are a block of a 4x4x8 slice.
Arguments:
- x_in: bfloat16 [2, 512, 2048], P(None, ('dp', 'tp'))
- y_cot: bfloat16 [2, 512, 2048], P(None, ('dp', 'tp'))
- gain_attn: float32 [2, 2048], replicated
- gain_mlp: float32 [2, 2048], replicated
- w_qkv: bfloat16 [2, 2048, 32, 3, 64], P(None, None, 'tp')
- w_out: bfloat16 [2, 32, 64, 2048], P(None, 'tp')
- w_gate: bfloat16 [2, 2048, 8192], P(None, None, 'tp')
- w_up: bfloat16 [2, 2048, 8192], P(None, None, 'tp')
- w_down: bfloat16 [2, 8192, 2048], P(None, 'tp')
Outputs:
- output 1: bfloat16 [2, 512, 2048], P(None, ('dp', 'tp'))
- output 2: bfloat16 [2, 512, 2048], P(None, ('dp', 'tp'))
- output 3: bfloat16 [2, 2048, 32, 3, 64], P('dp', None, 'tp')
- output 4: bfloat16 [2, 32, 64, 2048], P('dp', 'tp')
- output 5: bfloat16 [2, 2048, 8192], P('dp', None, 'tp')
- output 6: bfloat16 [2, 2048, 8192], P('dp', None, 'tp')
- output 7: bfloat16 [2, 8192, 2048], P('dp', 'tp')
- output 8: float32 [2, 2048], P('dp')
- output 9: float32 [2, 2048], P('dp')
All inputs are finite; a program needn't handle non-finite values.
Results may differ from the reference program's by a relative error of at most 0.02.
Values are sent between devices in bfloat16 or wider.
A program may use at most 768 MiB of HBM per device.

```python
import jax
import jax.numpy as jnp
from jax import lax

D = 2048
FF = 8192
HEADS = 32
KV_HEADS = 32
HEAD = 64
SEQ = 512
LAYERS = 2
MICRO = 2
GROUP = HEADS // KV_HEADS
NORM_EPS = 1e-5


def setup_inputs(seed: int = 0, part: int = 0) -> dict:
    base_key = jax.random.key(seed)
    shared_keys = jax.random.split(base_key, 7)
    part_keys = jax.random.split(jax.random.fold_in(base_key, part), 2)
    x_in = jax.random.normal(part_keys[0], (MICRO, SEQ, D), jnp.float32)
    y_cot = jax.random.normal(part_keys[1], (MICRO, SEQ, D), jnp.float32)
    gain_attn = 1.0 + 0.3 * jax.random.normal(shared_keys[0], (LAYERS, D), jnp.float32)
    gain_mlp = 1.0 + 0.3 * jax.random.normal(shared_keys[1], (LAYERS, D), jnp.float32)
    w_qkv = jax.random.normal(shared_keys[2], (LAYERS, D, KV_HEADS, GROUP + 2, HEAD), jnp.float32) * D ** -0.5
    w_out = jax.random.normal(shared_keys[3], (LAYERS, HEADS, HEAD, D), jnp.float32) * (HEADS * HEAD) ** -0.5
    w_gate = jax.random.normal(shared_keys[4], (LAYERS, D, FF), jnp.float32) * D ** -0.5
    w_up = jax.random.normal(shared_keys[5], (LAYERS, D, FF), jnp.float32) * D ** -0.5
    w_down = jax.random.normal(shared_keys[6], (LAYERS, FF, D), jnp.float32) * FF ** -0.5
    return {'x_in': x_in.astype(jnp.bfloat16), 'y_cot': y_cot.astype(jnp.bfloat16), 'gain_attn': gain_attn, 'gain_mlp': gain_mlp, 'w_qkv': w_qkv.astype(jnp.bfloat16), 'w_out': w_out.astype(jnp.bfloat16), 'w_gate': w_gate.astype(jnp.bfloat16), 'w_up': w_up.astype(jnp.bfloat16), 'w_down': w_down.astype(jnp.bfloat16)}


def rms_norm(row_vals, gain_vec):
    return row_vals * lax.rsqrt(jnp.mean(row_vals * row_vals, axis=-1, keepdims=True) + NORM_EPS) * gain_vec


def group_attention(queries, key_rows, value_rows):
    scores = jnp.einsum('qge,ke->gqk', queries.astype(jnp.float32), key_rows.astype(jnp.float32)) * HEAD ** -0.5
    positions = jnp.arange(SEQ)
    scores = jnp.where(positions[:, None] >= positions[None, :], scores, -1e30)
    prob_b16 = jax.nn.softmax(scores, axis=-1).astype(jnp.bfloat16)
    attn_mix = jnp.einsum('gqk,ke->qge', prob_b16.astype(jnp.float32), value_rows.astype(jnp.float32))
    return attn_mix.astype(jnp.bfloat16)


attention_ckpt = jax.checkpoint(group_attention)


def group_step(group_args):
    return attention_ckpt(group_args[0], group_args[1], group_args[2])


def layer_forward(layer_in, layer_params):
    gain_first, gain_second, qkv_weight, out_weight, gate_weight, up_weight, down_weight = layer_params
    x_f32 = layer_in.astype(jnp.float32)
    normed = rms_norm(x_f32, gain_first).astype(jnp.bfloat16)
    qkv_heads = jnp.einsum('sd,dkje->skje', normed.astype(jnp.float32), qkv_weight).astype(jnp.bfloat16)
    attn_mix = lax.map(group_step, (jnp.swapaxes(qkv_heads[:, :, :GROUP], 0, 1), jnp.swapaxes(qkv_heads[:, :, GROUP], 0, 1), jnp.swapaxes(qkv_heads[:, :, GROUP + 1], 0, 1)))
    attn_sum = jnp.einsum('kqge,kged->qd', attn_mix.astype(jnp.float32), out_weight.reshape(KV_HEADS, GROUP, HEAD, D))
    hidden = (x_f32 + attn_sum.astype(jnp.bfloat16).astype(jnp.float32)).astype(jnp.bfloat16)
    normed_b = rms_norm(hidden.astype(jnp.float32), gain_second).astype(jnp.bfloat16)
    gate_pre = jnp.dot(normed_b.astype(jnp.float32), gate_weight, preferred_element_type=jnp.float32)
    up_proj = jnp.dot(normed_b.astype(jnp.float32), up_weight, preferred_element_type=jnp.float32)
    inner = (jax.nn.silu(gate_pre) * up_proj).astype(jnp.bfloat16)
    down_sum = jnp.dot(inner.astype(jnp.float32), down_weight, preferred_element_type=jnp.float32).astype(jnp.bfloat16)
    return (hidden.astype(jnp.float32) + down_sum.astype(jnp.float32)).astype(jnp.bfloat16)


def stack_forward(layer_in, params):
    def layer_body(carry, layer_params):
        return layer_forward(carry, layer_params), None
    final_rows, unused = lax.scan(layer_body, layer_in, params)
    return final_rows


def reference(x_in, y_cot, gain_attn, gain_mlp, w_qkv, w_out, w_gate, w_up, w_down):
    params = (gain_attn, gain_mlp, w_qkv.astype(jnp.float32), w_out.astype(jnp.float32), w_gate.astype(jnp.float32), w_up.astype(jnp.float32), w_down.astype(jnp.float32))
    first_out, first_pull = jax.vjp(stack_forward, x_in[0], params)
    first_rows, first_grads = first_pull(y_cot[0])
    second_out, second_pull = jax.vjp(stack_forward, x_in[1], params)
    second_rows, second_grads = second_pull(y_cot[1])
    summed = [grad_one + grad_two for grad_one, grad_two in zip(first_grads, second_grads)]
    return (jnp.stack([first_out, second_out]), jnp.stack([first_rows, second_rows]), summed[2].astype(jnp.bfloat16), summed[3].astype(jnp.bfloat16), summed[4].astype(jnp.bfloat16), summed[5].astype(jnp.bfloat16), summed[6].astype(jnp.bfloat16), summed[0], summed[1])
```

```python
import functools
import math

import jax
import jax.numpy as jnp
from jax import lax
from jax.experimental import pallas as pl
from jax.experimental.pallas import tpu as pltpu
from jax.sharding import PartitionSpec as P

NORM_EPS = 1e-5
MESH = pl.DeviceIdType.MESH
CORES = 2
F32 = jnp.float32
B16 = jnp.bfloat16


def rms_scale(row_vals, gain_vec):
    return row_vals * lax.rsqrt(jnp.mean(row_vals * row_vals, axis=-1, keepdims=True) + NORM_EPS) * gain_vec


class Place:
    def __init__(self, side):
        me = lax.axis_index('tp')
        self.side = side
        self.core = lax.rem(me, CORES)
        chip = lax.div(me, CORES)
        self.x = lax.rem(chip, side)
        self.y = lax.div(chip, side)
        self.partner = self.dev(self.y, self.x, 1 - self.core)

    def dev(self, y, x, core):
        return {'tp': (y * self.side + x) * CORES + core}

    def shift(self, coord, by):
        return lax.rem(coord + by + self.side, self.side)

    def on_ring(self, axis, by):
        if axis == 0:
            return self.dev(self.y, self.shift(self.x, by), self.core)
        return self.dev(self.shift(self.y, by), self.x, self.core)


class Copies:
    def __init__(self, send_sems, recv_sems):
        self.send_sems = send_sems
        self.recv_sems = recv_sems
        self.started = []

    def start(self, src, dst, target):
        idx = len(self.started)
        copy = pltpu.make_async_remote_copy(src_ref=src, dst_ref=dst, send_sem=self.send_sems.at[idx],
                                            recv_sem=self.recv_sems.at[idx], device_id=target, device_id_type=MESH)
        copy.start()
        self.started.append(copy)
        return copy

    def finish(self):
        for copy in self.started:
            copy.wait_send()


def entry_barrier(place, far):
    targets = [place.partner]
    for axis in (0, 1):
        for by in (1, -1) + ((2,) if far else ()):
            targets.append(place.on_ring(axis, by))
    barrier = pltpu.get_barrier_semaphore()
    for target in targets:
        pl.semaphore_signal(barrier, inc=1, device_id=target, device_id_type=MESH)
    pl.semaphore_wait(barrier, len(targets))


def add_rows(dst, *terms):
    def body(i, carry):
        total = terms[0][i]
        for term in terms[1:]:
            total = total + term[i]
        dst[i] = total
        return carry
    lax.fori_loop(0, dst.shape[0], body, 0)


def reduce_scatter(place, copies, pairs, send_buf, own_buf, chip_buf, ring_buf, tail_buf, sums, mm_cols):
    side = place.side
    micro = sums.shape[0]
    rows = sums.shape[1]
    half_cols = sums.shape[2] // 2

    def products(half, core, buf):
        for m in range(micro):
            for start in range(0, half_cols, mm_cols):
                cols = pl.ds(half * half_cols + start, mm_cols)
                total = None
                for a_ref, b_ref, transposed in pairs:
                    left = a_ref[m, core]
                    if transposed:
                        part = lax.dot_general(left, b_ref[cols, :], (((1,), (1,)), ((), ())), preferred_element_type=F32)
                    else:
                        part = jnp.dot(left, b_ref[:, cols], preferred_element_type=F32)
                    total = part if total is None else total + part
                total = total.reshape(side, side, rows, mm_cols)
                for yy in range(side):
                    for xx in range(side):
                        first, second = (xx, yy) if half == 0 else (yy, xx)
                        buf[half, first, m, second, :, start:start + mm_cols] = total[yy, xx]

    spots = []
    chip_copies = {}
    for half in (0, 1):
        coord = place.x if half == 0 else place.y
        spots.append((coord, place.shift(coord, 1), place.shift(coord, -1), place.shift(coord, 2)))
    for half in (0, 1):
        products(half, 1 - place.core, send_buf)
        here, plus, minus, far = spots[half]
        for name, spot in (('far', far), ('plus', plus), ('minus', minus), ('here', here)):
            chip_copies[half, name] = copies.start(send_buf.at[half, spot], chip_buf.at[half, spot], place.partner)
    for half in (0, 1):
        products(half, place.core, own_buf)

    def join(half, name, spot):
        chip_copies[half, name].wait_recv()
        for m in range(micro):
            add_rows(own_buf.at[half, spot, m], own_buf.at[half, spot, m], chip_buf.at[half, spot, m])

    first = {}
    for half in (0, 1):
        here, plus, minus, far = spots[half]
        join(half, 'far', far)
        first[half, 0] = copies.start(own_buf.at[half, far, 0], ring_buf.at[half, 0], place.on_ring(half, 1))
        first[half, 1] = copies.start(own_buf.at[half, far, 1], ring_buf.at[half, 1], place.on_ring(half, -1))
    for half in (0, 1):
        here, plus, minus, far = spots[half]
        join(half, 'plus', plus)
        first[half, 2] = copies.start(own_buf.at[half, plus, 1], ring_buf.at[half, 2], place.on_ring(half, 1))
        join(half, 'minus', minus)
        first[half, 3] = copies.start(own_buf.at[half, minus, 0], ring_buf.at[half, 3], place.on_ring(half, -1))
    for half in (0, 1):
        join(half, 'here', spots[half][0])
    for half in (0, 1):
        here, plus, minus, far = spots[half]
        first[half, 0].wait_recv()
        add_rows(own_buf.at[half, plus, 0], own_buf.at[half, plus, 0], ring_buf.at[half, 0])
        first[half, 4] = copies.start(own_buf.at[half, plus, 0], ring_buf.at[half, 4], place.on_ring(half, 1))
        first[half, 1].wait_recv()
        add_rows(own_buf.at[half, minus, 1], own_buf.at[half, minus, 1], ring_buf.at[half, 1])
        first[half, 5] = copies.start(own_buf.at[half, minus, 1], ring_buf.at[half, 5], place.on_ring(half, -1))
    second = {}
    for half in (0, 1):
        here = spots[half][0]
        axis = 1 - half
        _, plus, minus, far = spots[axis]
        for slot in (2, 3, 4, 5):
            first[half, slot].wait_recv()
        add_rows(own_buf.at[half, here, 0], own_buf.at[half, here, 0], ring_buf.at[half, 3], ring_buf.at[half, 4])
        add_rows(own_buf.at[half, here, 1], own_buf.at[half, here, 1], ring_buf.at[half, 2], ring_buf.at[half, 5])
        second[half, 0] = copies.start(own_buf.at[half, here, 0, far], tail_buf.at[half, 0], place.on_ring(axis, 1))
        second[half, 1] = copies.start(own_buf.at[half, here, 1, far], tail_buf.at[half, 1], place.on_ring(axis, -1))
        second[half, 2] = copies.start(own_buf.at[half, here, 1, plus], tail_buf.at[half, 2], place.on_ring(axis, 1))
        second[half, 3] = copies.start(own_buf.at[half, here, 0, minus], tail_buf.at[half, 3], place.on_ring(axis, -1))
    for half in (0, 1):
        here = spots[half][0]
        axis = 1 - half
        _, plus, minus, _ = spots[axis]
        second[half, 0].wait_recv()
        own_buf[half, here, 0, plus] = own_buf[half, here, 0, plus] + tail_buf[half, 0]
        second[half, 4] = copies.start(own_buf.at[half, here, 0, plus], tail_buf.at[half, 4], place.on_ring(axis, 1))
        second[half, 1].wait_recv()
        own_buf[half, here, 1, minus] = own_buf[half, here, 1, minus] + tail_buf[half, 1]
        second[half, 5] = copies.start(own_buf.at[half, here, 1, minus], tail_buf.at[half, 5], place.on_ring(axis, -1))
    for half in (0, 1):
        here = spots[half][0]
        mine = spots[1 - half][0]
        cols = slice(half * half_cols, (half + 1) * half_cols)
        for slot in (2, 3, 4, 5):
            second[half, slot].wait_recv()
        sums[0, :, cols] = own_buf[half, here, 0, mine] + tail_buf[half, 3] + tail_buf[half, 4]
        sums[1, :, cols] = own_buf[half, here, 1, mine] + tail_buf[half, 2] + tail_buf[half, 5]


def all_gather(place, copies, fulls):
    core = place.core
    half_cols = fulls[0].shape[-1] // 2
    coords = (place.x, place.y)
    jobs = [(full, half) for full in fulls for half in (0, 1)]

    def piece(full, half, spot, other, micro):
        yy, xx = (other, spot) if half == 0 else (spot, other)
        cols = pl.ds(half * half_cols, half_cols)
        if micro is None:
            return full.at[:, core, yy, xx, :, cols]
        return full.at[micro, core, yy, xx, :, cols]

    def line(full, half, other):
        cols = pl.ds(half * half_cols, half_cols)
        if half == 0:
            return full.at[:, core, other, :, :, cols]
        return full.at[:, core, :, other, :, cols]

    def send(full, half, spot, other, micro, axis, by):
        ref = piece(full, half, spot, other, micro)
        return copies.start(ref, ref, place.on_ring(axis, by))

    def send_line(full, half, other):
        ref = line(full, half, other)
        return copies.start(ref, ref, place.partner)

    first, second, last = {}, {}, []
    for j, (full, half) in enumerate(jobs):
        spot, other = coords[half], coords[1 - half]
        for by in (1, -1):
            first[j, by] = send(full, half, spot, other, None, half, by)
        for by in (1, -1):
            second[j, 0, by] = send(full, half, spot, other, None, 1 - half, by)
    for j, (full, half) in enumerate(jobs):
        spot, other = coords[half], coords[1 - half]
        for by, micro in ((1, 0), (-1, 1)):
            first[j, by].wait_recv()
            came = place.shift(spot, -by)
            first[j, by, 'far'] = send(full, half, came, other, micro, half, by)
            for to in (1, -1):
                second[j, -by, to] = send(full, half, came, other, None, 1 - half, to)
    for j, (full, half) in enumerate(jobs):
        spot, other = coords[half], coords[1 - half]
        for by in (1, -1):
            first[j, by, 'far'].wait_recv()
        far = place.shift(spot, 2)
        for to in (1, -1):
            second[j, 2, to] = send(full, half, far, other, None, 1 - half, to)
        last.append(send_line(full, half, other))
    tails = {}
    for off in (0, 1, -1, 2):
        for j, (full, half) in enumerate(jobs):
            spot, other = coords[half], coords[1 - half]
            for to, micro in ((1, 0), (-1, 1)):
                second[j, off, to].wait_recv()
                came = place.shift(other, -to)
                tails[j, off, to] = send(full, half, place.shift(spot, off), came, micro, 1 - half, to)
    for j, (full, half) in enumerate(jobs):
        for to in (1, -1):
            last.append(send_line(full, half, place.shift(coords[1 - half], to)))
    for j, (full, half) in enumerate(jobs):
        for off in (0, 1, -1, 2):
            for to in (1, -1):
                tails[j, off, to].wait_recv()
        last.append(send_line(full, half, place.shift(coords[1 - half], 2)))
    for copy in last:
        copy.wait_recv()


def all_reduce(place, copies, value, pair_buf, ring_bufs, out):
    side = place.side
    copy = copies.start(value, pair_buf, place.partner)
    copy.wait_recv()
    total = value[...] + pair_buf[...]
    for axis in (0, 1):
        coord = place.x if axis == 0 else place.y
        buf = ring_bufs.at[axis]
        buf[coord] = total
        going = [copies.start(buf.at[coord], buf.at[coord], place.on_ring(axis, by)) for by in (1, -1, 2)]
        for copy in going:
            copy.wait_recv()
        total = buf[0]
        for k in range(1, side):
            total = total + buf[k]
    out[...] = total


def epilogue_forward(sums, residual, gain):
    row_sum = residual[...].astype(F32) + sums[...].astype(B16).astype(F32)
    new_rows = row_sum.astype(B16)
    normed = rms_scale(new_rows.astype(F32), gain[...].reshape(1, 1, -1)).astype(B16)
    return new_rows, normed


def epilogue_backward(sums, rows_in, gain, cot):
    vals = rows_in[...].astype(F32)
    grad = sums[...].astype(B16).astype(F32)
    inv = lax.rsqrt(jnp.mean(vals * vals, axis=-1, keepdims=True) + NORM_EPS)
    unit = vals * inv
    scaled = grad * gain[...].reshape(1, 1, -1)
    back = inv * (scaled - unit * jnp.mean(scaled * unit, axis=-1, keepdims=True))
    new_cot = (cot[...].astype(F32) + back).astype(B16)
    return new_cot, jnp.sum(jnp.sum(grad * unit, axis=0), axis=0, keepdims=True)


def stage_call(side, cid, kind, left, right, transposed, row_ins, gain, extra, grads):
    micro, rows, width = row_ins[0].shape
    half_cols = width // 2
    shard = jax.ShapeDtypeStruct((micro, rows, width), B16)
    full = jax.ShapeDtypeStruct((micro, CORES, side, side, rows, width), B16)
    part = jax.ShapeDtypeStruct((1, width), F32)
    reduces = kind != 'norm'
    new_full = kind in ('norm', 'fwd', 'bwd')
    outs = {'norm': [shard], 'fwd': [shard, shard], 'fwd_last': [shard], 'bwd': [shard, part], 'bwd_last': [shard]}[kind]
    n_small = len(outs)
    n_full = len(extra) + new_full
    outs = outs + [full] * n_full
    total_reduce = kind == 'bwd_last'
    n_terms = len(grads) + 1
    if total_reduce:
        outs = outs + [jax.ShapeDtypeStruct((2 * CORES * CORES, width), F32)]
    scratch = []
    if reduces:
        piece = (2, side, micro, side, rows, half_cols)
        scratch += [pltpu.VMEM(piece, F32)] * 3
        scratch += [pltpu.VMEM((2, 6, side, rows, half_cols), F32), pltpu.VMEM((2, 6, rows, half_cols), F32),
                    pltpu.VMEM((micro, rows, width), F32)]
    if total_reduce:
        scratch += [pltpu.VMEM((8, width), F32), pltpu.VMEM((8, width), F32), pltpu.VMEM((2, side, 8, width), F32)]
    n_sems = 48 * n_full + (32 if reduces else 0) + (7 if total_reduce else 0)
    scratch += [pltpu.SemaphoreType.DMA((n_sems,)), pltpu.SemaphoreType.DMA((n_sems,))]
    n_pair = len(left)
    n_rows, n_extra, n_grads = len(row_ins), len(extra), len(grads)
    has_gain = gain is not None

    def body(*refs):
        refs = list(refs)

        def take(count):
            got, refs[:] = refs[:count], refs[count:]
            return got
        lefts, rights, row_refs = take(n_pair), take(n_pair), take(n_rows)
        gain_ref = take(1)[0] if has_gain else None
        extra_refs, grad_refs = take(n_extra), take(n_grads)
        small_outs, full_outs = take(n_small), take(n_full)
        total_out = take(1)[0] if total_reduce else None
        if reduces:
            send_buf, own_buf, chip_buf, ring_buf, tail_buf, sums = take(6)
        if total_reduce:
            value, pair_buf, ring_bufs = take(3)
        send_sems, recv_sems = take(2)
        place = Place(side)
        copies = Copies(send_sems, recv_sems)
        entry_barrier(place, total_reduce)
        for ref, out in zip(extra_refs, full_outs):
            out[:, place.core, place.y, place.x] = ref[...]
        if reduces:
            pairs = list(zip(lefts, rights, [transposed] * n_pair))
            reduce_scatter(place, copies, pairs, send_buf, own_buf, chip_buf, ring_buf, tail_buf, sums, min(512, half_cols))
        new = None
        if kind == 'norm':
            new = rms_scale(row_refs[0][...].astype(F32), gain_ref[...].reshape(1, 1, -1)).astype(B16)
            small_outs[0][...] = new
        elif kind == 'fwd':
            new_rows, new = epilogue_forward(sums, row_refs[0], gain_ref)
            small_outs[0][...] = new_rows
            small_outs[1][...] = new
        elif kind == 'fwd_last':
            small_outs[0][...] = (row_refs[0][...].astype(F32) + sums[...].astype(B16).astype(F32)).astype(B16)
        else:
            new, gain_part = epilogue_backward(sums, row_refs[0], gain_ref, row_refs[1])
            small_outs[0][...] = new
            if total_reduce:
                value[...] = jnp.zeros_like(value)
                for i, ref in enumerate(grad_refs):
                    value[i:i + 1] = ref[...]
                value[n_terms - 1:n_terms] = gain_part
            else:
                small_outs[1][...] = gain_part
        if new_full:
            full_outs[-1][:, place.core, place.y, place.x] = new
        if full_outs:
            all_gather(place, copies, full_outs)
        if total_reduce:
            all_reduce(place, copies, value, pair_buf, ring_bufs, total_out)
        copies.finish()

    ins = list(left) + list(right) + list(row_ins) + ([gain.reshape(1, width)] if has_gain else []) + list(extra) + list(grads)
    vmem = pl.BlockSpec(memory_space=pltpu.VMEM)
    return pl.pallas_call(
        body, out_shape=outs, in_specs=[vmem] * len(ins), out_specs=[vmem] * len(outs), scratch_shapes=scratch,
        compiler_params=pltpu.CompilerParams(collective_id=cid, has_side_effects=True),
        name=f'stage_{kind}_{cid}')(*ins)


def attention_forward(queries, key_heads, value_heads, mask, score_scale):
    scores = jnp.einsum('mqe,mte->mqt', queries, key_heads, preferred_element_type=F32) * score_scale
    scores = jnp.where(mask, scores, -1e30)
    row_max = jnp.max(scores, axis=-1, keepdims=True)
    exp_scores = jnp.exp(scores - row_max)
    row_total = jnp.sum(exp_scores, axis=-1, keepdims=True)
    prob_b16 = (exp_scores / row_total).astype(B16)
    attn_mix = jnp.einsum('mqt,mte->mqe', prob_b16, value_heads, preferred_element_type=F32).astype(B16)
    return attn_mix, row_max + jnp.log(row_total)


def attention_backward(queries, key_heads, value_heads, log_norm, grad_mix, mask, score_scale):
    scores = jnp.einsum('mqe,mte->mqt', queries, key_heads, preferred_element_type=F32) * score_scale
    scores = jnp.where(mask, scores, -1e30)
    prob_f32 = jnp.exp(scores - log_norm)
    prob_b16 = prob_f32.astype(B16)
    grad_prob = jnp.einsum('mqe,mte->mqt', grad_mix, value_heads, preferred_element_type=F32).astype(B16).astype(F32)
    row_dot = jnp.sum(grad_prob * prob_f32, axis=-1, keepdims=True)
    grad_scores = (prob_f32 * (grad_prob - row_dot) * score_scale).astype(B16)
    grad_q = jnp.einsum('mqt,mte->mqe', grad_scores, key_heads, preferred_element_type=F32)
    grad_k = jnp.einsum('mqt,mqe->mte', grad_scores, queries, preferred_element_type=F32)
    grad_v = jnp.einsum('mqt,mqe->mte', prob_b16, grad_mix, preferred_element_type=F32)
    return grad_q, grad_k, grad_v


def solution(mesh):
    row_spec = P(None, ('dp', 'tp'), None)
    gain_spec = P(None, None)
    qkv_spec = P(None, None, 'tp', None, None)
    head_spec = P(None, 'tp', None, None)
    col_spec = P(None, None, 'tp')
    row_shard_spec = P(None, 'tp', None)
    side = math.isqrt(mesh.shape['tp'] // CORES)

    def device_program(x_in, y_cot, gain_attn, gain_mlp, w_qkv, w_out, w_gate, w_up, w_down):
        micro, rows, width = x_in.shape
        layer_count = w_qkv.shape[0]
        slots = w_qkv.shape[2] * w_qkv.shape[3]
        head_dim = w_qkv.shape[4]
        assert slots == 3 and side == 4 and micro == 2
        score_scale = head_dim ** -0.5
        seq = rows * side * side * CORES
        qkv_flat = w_qkv.reshape(layer_count, width, slots * head_dim)
        out_flat = w_out.reshape(layer_count, head_dim, width)
        pos = jnp.arange(seq, dtype=jnp.int32).reshape(side * side, CORES, rows).swapaxes(0, 1).reshape(seq)
        mask = (pos[:, None] >= pos[None, :])[None]
        call_ids = iter(range(64))

        def stage(kind, left=(), right=(), transposed=False, row_ins=(), gain=None, extra=(), grads=()):
            left = [item.reshape(micro, CORES, side * side * rows, item.shape[-1]) for item in left]
            return stage_call(side, next(call_ids), kind, left, list(right), transposed, list(row_ins), gain, list(extra), list(grads))

        def flat(full):
            return full.reshape(micro * seq, width)

        def dot(a, b, ca, cb):
            return lax.dot_general(a, b, (((ca,), (cb,)), ((), ())), preferred_element_type=F32)

        kept = []
        rows_x = x_in
        normed, full_u = stage('norm', row_ins=[x_in], gain=gain_attn[0])
        for layer in range(layer_count):
            qkv = dot(flat(full_u), qkv_flat[layer], 1, 0).astype(B16).reshape(micro, seq, slots * head_dim)
            queries, keys, values = (qkv[..., i * head_dim:(i + 1) * head_dim] for i in range(slots))
            attn_mix, log_norm = attention_forward(queries, keys, values, mask, score_scale)
            hidden, normed_b, full_v = stage('fwd', [attn_mix], [out_flat[layer]], False, [rows_x], gain_mlp[layer])
            gate_pre = dot(flat(full_v), w_gate[layer], 1, 0)
            up_proj = dot(flat(full_v), w_up[layer], 1, 0)
            inner = (jax.nn.silu(gate_pre) * up_proj).astype(B16)
            kept.append((rows_x, normed, hidden, normed_b, queries, keys, values, attn_mix, log_norm))
            if layer + 1 < layer_count:
                rows_x, normed, full_u = stage('fwd', [inner], [w_down[layer]], False, [hidden], gain_attn[layer + 1])
            else:
                rows_y, full_v, full_g = stage('fwd_last', [inner], [w_down[layer]], False, [hidden], None, [normed_b, y_cot])

        grad_rows = y_cot
        out_grads = [[None] * layer_count for _ in range(5)]
        gain_parts = {}
        for layer in reversed(range(layer_count)):
            rows_x, normed, hidden, normed_b, queries, keys, values, attn_mix, log_norm = kept[layer]
            flat_v, flat_g = flat(full_v), flat(full_g)
            gate_pre = dot(flat_v, w_gate[layer], 1, 0)
            up_proj = dot(flat_v, w_up[layer], 1, 0)
            gate_sig = jax.nn.sigmoid(gate_pre)
            gate_act = gate_pre * gate_sig
            inner = (gate_act * up_proj).astype(B16)
            out_grads[4][layer] = dot(inner, flat_g, 0, 0).astype(B16)
            grad_inner = dot(flat_g, w_down[layer], 1, 1).astype(B16).astype(F32)
            grad_up = (grad_inner * gate_act).astype(B16)
            grad_gate = (grad_inner * up_proj * gate_sig * (1.0 + gate_pre * (1.0 - gate_sig))).astype(B16)
            out_grads[2][layer] = dot(flat_v, grad_gate, 0, 0).astype(B16)
            out_grads[3][layer] = dot(flat_v, grad_up, 0, 0).astype(B16)
            grad_hidden, gain_parts['mlp', layer], full_u, full_gh = stage(
                'bwd', [grad_gate, grad_up], [w_gate[layer], w_up[layer]], True, [hidden, grad_rows], gain_mlp[layer], [normed])
            flat_u, flat_gh = flat(full_u), flat(full_gh)
            flat_mix = attn_mix.reshape(micro * seq, head_dim)
            out_grads[1][layer] = dot(flat_mix, flat_gh, 0, 0).astype(B16)
            grad_mix = dot(flat_gh, out_flat[layer], 1, 1).astype(B16).reshape(micro, seq, head_dim)
            grad_qkv = jnp.concatenate(attention_backward(queries, keys, values, log_norm, grad_mix, mask, score_scale), axis=-1).astype(B16)
            out_grads[0][layer] = dot(flat_u, grad_qkv.reshape(micro * seq, slots * head_dim), 0, 0).astype(B16)
            if layer > 0:
                grad_rows, gain_parts['attn', layer], full_v, full_g = stage(
                    'bwd', [grad_qkv], [qkv_flat[layer]], True, [rows_x, grad_hidden], gain_attn[layer], [kept[layer - 1][3]])
            else:
                terms = [gain_parts['attn', item] for item in range(1, layer_count)] + [gain_parts['mlp', item] for item in range(layer_count)]
                grad_rows, gain_sums = stage(
                    'bwd_last', [grad_qkv], [qkv_flat[layer]], True, [rows_x, grad_hidden], gain_attn[layer], [], terms)
        n_attn = layer_count - 1
        gain_a = jnp.concatenate([gain_sums[2 * layer_count - 1:2 * layer_count], gain_sums[:n_attn]], axis=0)
        gain_b = gain_sums[n_attn:n_attn + layer_count]
        return (rows_y, grad_rows,
                jnp.stack(out_grads[0]).reshape(w_qkv.shape), jnp.stack(out_grads[1]).reshape(w_out.shape),
                jnp.stack(out_grads[2]), jnp.stack(out_grads[3]), jnp.stack(out_grads[4]), gain_a, gain_b)

    return jax.shard_map(device_program, mesh=mesh,
                         in_specs=(row_spec, row_spec, gain_spec, gain_spec, qkv_spec, head_spec, col_spec, col_spec, row_shard_spec),
                         out_specs=(row_spec, row_spec, P('dp', None, 'tp', None, None), P('dp', 'tp', None, None), P('dp', None, 'tp'), P('dp', None, 'tp'), P('dp', 'tp', None), P('dp', None), P('dp', None)),
                         check_vma=False)
```

```python
import functools
import math

import jax
import jax.numpy as jnp
from jax import lax
from jax.experimental import pallas as pl
from jax.experimental.pallas import tpu as pltpu
from jax.sharding import PartitionSpec as P

NORM_EPS = 1e-5
MESH = pl.DeviceIdType.MESH
CORES = 2
F32 = jnp.float32
B16 = jnp.bfloat16


def rms_scale(row_vals, gain_vec):
    return row_vals * lax.rsqrt(jnp.mean(row_vals * row_vals, axis=-1, keepdims=True) + NORM_EPS) * gain_vec


class Place:
    def __init__(self, side):
        me = lax.axis_index('tp')
        self.side = side
        self.core = lax.rem(me, CORES)
        chip = lax.div(me, CORES)
        self.x = lax.rem(chip, side)
        self.y = lax.div(chip, side)
        self.partner = self.dev(self.y, self.x, 1 - self.core)

    def dev(self, y, x, core):
        return {'tp': (y * self.side + x) * CORES + core}

    def shift(self, coord, by):
        return lax.rem(coord + by + self.side, self.side)

    def on_ring(self, axis, by):
        if axis == 0:
            return self.dev(self.y, self.shift(self.x, by), self.core)
        return self.dev(self.shift(self.y, by), self.x, self.core)


class Copies:
    def __init__(self, send_sems, recv_sems):
        self.send_sems = send_sems
        self.recv_sems = recv_sems
        self.started = []

    def start(self, src, dst, target):
        idx = len(self.started)
        copy = pltpu.make_async_remote_copy(src_ref=src, dst_ref=dst, send_sem=self.send_sems.at[idx],
                                            recv_sem=self.recv_sems.at[idx], device_id=target, device_id_type=MESH)
        copy.start()
        self.started.append(copy)
        return copy

    def finish(self):
        for copy in self.started:
            copy.wait_send()


def entry_barrier(place):
    targets = [place.partner] + [place.on_ring(axis, by) for axis in (0, 1) for by in (1, -1, 2)]
    barrier = pltpu.get_barrier_semaphore()
    for target in targets:
        pl.semaphore_signal(barrier, inc=1, device_id=target, device_id_type=MESH)
    return lambda: pl.semaphore_wait(barrier, len(targets))


def add_rows(dst, *terms):
    def body(i, carry):
        total = terms[0][i]
        for term in terms[1:]:
            total = total + term[i]
        dst[i] = total
        return carry
    lax.fori_loop(0, dst.shape[0], body, 0)


class ReduceScatter:
    def __init__(self, place, copies, pairs, m, send_buf, own_buf, chip_buf, ring_buf, tail_buf, sums):
        self.place, self.copies, self.pairs, self.m = place, copies, pairs, m
        self.send_buf, self.own_buf, self.chip_buf, self.ring_buf, self.tail_buf, self.sums = (
            ref.at[m] for ref in (send_buf, own_buf, chip_buf, ring_buf, tail_buf, sums))
        self.quarter = self.own_buf.shape[-1]
        self.rows = self.own_buf.shape[-2]
        self.spots = [(coord, place.shift(coord, 1), place.shift(coord, -1), place.shift(coord, 2))
                      for coord in (place.x, place.y)]
        self.chip_copies, self.first, self.second = {}, {}, {}

    def products(self, half, core, buf):
        side, rows, quarter = self.place.side, self.rows, self.quarter

        def one(sub, carry):
            cols = pl.ds(pl.multiple_of((half * 2 + sub) * quarter, quarter), quarter)
            total = None
            for a_ref, b_ref, transposed in self.pairs:
                left = a_ref[self.m, :, core].reshape(side * side * rows, a_ref.shape[-1])
                if transposed:
                    part = lax.dot_general(left, b_ref[cols, :], (((1,), (1,)), ((), ())), preferred_element_type=F32)
                else:
                    part = jnp.dot(left, b_ref[:, cols], preferred_element_type=F32)
                total = part if total is None else total + part
            total = total.reshape(side, side, rows, quarter)
            for yy in range(side):
                for xx in range(side):
                    first, second = (xx, yy) if half == 0 else (yy, xx)
                    buf[half, first, sub, second] = total[yy, xx]
            return carry
        lax.fori_loop(0, 2, one, 0)

    def p0(self, entered=None):
        for half in (0, 1):
            self.products(half, 1 - self.place.core, self.send_buf)
            if entered is not None and half == 0:
                entered()
            self.to_partner(half, 'far', self.spots[half][3])
        for half in (0, 1):
            here, plus, minus, far = self.spots[half]
            for name, spot in (('plus', plus), ('minus', minus), ('here', here)):
                self.to_partner(half, name, spot)

    def to_partner(self, half, name, spot):
        self.chip_copies[half, name] = self.copies.start(self.send_buf.at[half, spot], self.chip_buf.at[half, spot], self.place.partner)

    def p1(self):
        for half in (0, 1):
            self.products(half, self.place.core, self.own_buf)

    def join(self, half, name, spot):
        self.chip_copies[half, name].wait_recv()
        for sub in (0, 1):
            add_rows(self.own_buf.at[half, spot, sub], self.own_buf.at[half, spot, sub], self.chip_buf.at[half, spot, sub])

    def ring(self, half, slot, spot, sub, by):
        self.first[half, slot] = self.copies.start(self.own_buf.at[half, spot, sub], self.ring_buf.at[half, slot], self.place.on_ring(half, by))

    def tail(self, half, slot, spot, sub, by):
        here = self.spots[half][0]
        self.second[half, slot] = self.copies.start(self.own_buf.at[half, here, sub, spot], self.tail_buf.at[half, slot],
                                                    self.place.on_ring(1 - half, by))

    def p2(self):
        for half in (0, 1):
            far = self.spots[half][3]
            self.join(half, 'far', far)
            self.ring(half, 0, far, 0, 1)
            self.ring(half, 1, far, 1, -1)

    def p3(self):
        for half in (0, 1):
            here, plus, minus, far = self.spots[half]
            self.join(half, 'plus', plus)
            self.ring(half, 2, plus, 1, 1)
            self.join(half, 'minus', minus)
            self.ring(half, 3, minus, 0, -1)
        for half in (0, 1):
            self.join(half, 'here', self.spots[half][0])

    def p4(self):
        own, ring = self.own_buf, self.ring_buf
        for half in (0, 1):
            here, plus, minus, far = self.spots[half]
            self.first[half, 0].wait_recv()
            add_rows(own.at[half, plus, 0], own.at[half, plus, 0], ring.at[half, 0])
            self.ring(half, 4, plus, 0, 1)
            self.first[half, 1].wait_recv()
            add_rows(own.at[half, minus, 1], own.at[half, minus, 1], ring.at[half, 1])
            self.ring(half, 5, minus, 1, -1)

    def p5(self):
        own, ring = self.own_buf, self.ring_buf
        for half in (0, 1):
            here = self.spots[half][0]
            _, plus, minus, far = self.spots[1 - half]
            for slot in (2, 3, 4, 5):
                self.first[half, slot].wait_recv()
            add_rows(own.at[half, here, 0], own.at[half, here, 0], ring.at[half, 3], ring.at[half, 4])
            add_rows(own.at[half, here, 1], own.at[half, here, 1], ring.at[half, 2], ring.at[half, 5])
            self.tail(half, 0, far, 0, 1)
            self.tail(half, 1, far, 1, -1)
            self.tail(half, 2, plus, 1, 1)
            self.tail(half, 3, minus, 0, -1)

    def p6(self):
        own, tail = self.own_buf, self.tail_buf
        for half in (0, 1):
            here = self.spots[half][0]
            _, plus, minus, _ = self.spots[1 - half]
            self.second[half, 0].wait_recv()
            own[half, here, 0, plus] = own[half, here, 0, plus] + tail[half, 0]
            self.tail(half, 4, plus, 0, 1)
            self.second[half, 1].wait_recv()
            own[half, here, 1, minus] = own[half, here, 1, minus] + tail[half, 1]
            self.tail(half, 5, minus, 1, -1)

    def p7(self):
        own, tail, quarter = self.own_buf, self.tail_buf, self.quarter
        for half in (0, 1):
            here, mine = self.spots[half][0], self.spots[1 - half][0]
            for slot in (2, 3, 4, 5):
                self.second[half, slot].wait_recv()
            start = half * 2 * quarter
            self.sums[:, start:start + quarter] = own[half, here, 0, mine] + tail[half, 3] + tail[half, 4]
            self.sums[:, start + quarter:start + 2 * quarter] = own[half, here, 1, mine] + tail[half, 2] + tail[half, 5]


class AllGather:
    def __init__(self, place, copies, arrays):
        self.place, self.copies = place, copies
        self.coords = (place.x, place.y)
        self.jobs = [(array, half) for array in arrays for half in (0, 1)]
        self.first, self.second, self.tails, self.last = {}, {}, {}, []

    def send(self, job, spot, other, sub, axis, by):
        array, half = job
        yy, xx = (other, spot) if half == 0 else (spot, other)
        half_cols = array.shape[-1] // 2
        cols = pl.ds(half * half_cols, half_cols) if sub is None else pl.ds(half * half_cols + sub * half_cols // 2, half_cols // 2)
        ref = array.at[yy, xx, self.place.core, :, cols]
        return self.copies.start(ref, ref, self.place.on_ring(axis, by))

    def send_line(self, job, other):
        array, half = job
        half_cols = array.shape[-1] // 2
        cols = pl.ds(half * half_cols, half_cols)
        core = self.place.core
        ref = array.at[other, :, core, :, cols] if half == 0 else array.at[:, other, core, :, cols]
        self.last.append(self.copies.start(ref, ref, self.place.partner))

    def each(self):
        for j, job in enumerate(self.jobs):
            half = job[1]
            yield j, job, half, self.coords[half], self.coords[1 - half]

    def a0(self):
        for j, job, half, spot, other in self.each():
            for by in (1, -1, 2):
                self.first[j, by] = self.send(job, spot, other, None, half, by)
            for by in (1, -1):
                self.second[j, 0, by] = self.send(job, spot, other, None, 1 - half, by)

    def a1(self):
        for j, job, half, spot, other in self.each():
            for by in (1, -1):
                self.first[j, by].wait_recv()
                came = self.place.shift(spot, -by)
                for to in (1, -1):
                    self.second[j, -by, to] = self.send(job, came, other, None, 1 - half, to)

    def a2(self):
        for j, job, half, spot, other in self.each():
            self.first[j, 2].wait_recv()
            far = self.place.shift(spot, 2)
            for to in (1, -1):
                self.second[j, 2, to] = self.send(job, far, other, None, 1 - half, to)
            self.send_line(job, other)

    def a3(self):
        for off in (0, 1, -1):
            self.pass_on(off)

    def pass_on(self, off):
        for j, job, half, spot, other in self.each():
            for to, sub in ((1, 0), (-1, 1)):
                self.second[j, off, to].wait_recv()
                came = self.place.shift(other, -to)
                self.tails[j, off, to] = self.send(job, self.place.shift(spot, off), came, sub, 1 - half, to)

    def a4(self):
        self.pass_on(2)
        for j, job, half, spot, other in self.each():
            for to in (1, -1):
                self.send_line(job, self.place.shift(other, to))

    def a5(self):
        for j, job, half, spot, other in self.each():
            for off in (0, 1, -1, 2):
                for to in (1, -1):
                    self.tails[j, off, to].wait_recv()
            self.send_line(job, self.place.shift(other, 2))

    def a6(self):
        for copy in self.last:
            copy.wait_recv()


def all_reduce(place, copies, value, pair_buf, ring_bufs, out):
    side = place.side
    copy = copies.start(value, pair_buf, place.partner)
    copy.wait_recv()
    total = value[...] + pair_buf[...]
    for axis in (0, 1):
        coord = place.x if axis == 0 else place.y
        buf = ring_bufs.at[axis]
        buf[coord] = total
        going = [copies.start(buf.at[coord], buf.at[coord], place.on_ring(axis, by)) for by in (1, -1, 2)]
        for copy in going:
            copy.wait_recv()
        total = buf[0]
        for k in range(1, side):
            total = total + buf[k]
    out[...] = total


def epilogue_forward(sums, residual, gain):
    new_rows = (residual.astype(F32) + sums.astype(B16).astype(F32)).astype(B16)
    return new_rows, rms_scale(new_rows.astype(F32), gain).astype(B16)


def epilogue_backward(sums, rows_in, gain, cot):
    vals = rows_in.astype(F32)
    grad = sums.astype(B16).astype(F32)
    inv = lax.rsqrt(jnp.mean(vals * vals, axis=-1, keepdims=True) + NORM_EPS)
    unit = vals * inv
    scaled = grad * gain
    back = inv * (scaled - unit * jnp.mean(scaled * unit, axis=-1, keepdims=True))
    new_cot = (cot.astype(F32) + back).astype(B16)
    return new_cot, jnp.sum(grad * unit, axis=0, keepdims=True)


def mm(a, b, ca, cb):
    return lax.dot_general(a, b, (((ca,), (cb,)), ((), ())), preferred_element_type=F32)


def rows_of(full, m):
    got = full[m]
    return got.reshape(-1, got.shape[-1])


def causal(scores, start):
    row = lax.broadcasted_iota(jnp.int32, scores.shape, 0) + start
    col = lax.broadcasted_iota(jnp.int32, scores.shape, 1)
    return jnp.where(row >= col, scores, -1e30)


def attention_forward(m, full, w_qkv, outs, scale, block):
    q_out, k_out, v_out, o_out, norm_out = outs
    rows = rows_of(full, m)
    for i, out in enumerate((q_out, k_out, v_out)):
        out[m] = mm(rows, w_qkv[i], 1, 1).astype(B16)
    for start in range(0, rows.shape[0], block):
        stop = start + block
        scores = causal(mm(q_out[m, start:stop], k_out[m, :stop], 1, 1) * scale, start)
        row_max = jnp.max(scores, axis=-1, keepdims=True)
        exp_scores = jnp.exp(scores - row_max)
        row_total = jnp.sum(exp_scores, axis=-1, keepdims=True)
        prob = (exp_scores / row_total).astype(B16)
        o_out[m, start:stop] = mm(prob, v_out[m, :stop], 1, 0).astype(B16)
        norm_out[m, start:stop] = jnp.broadcast_to(row_max + jnp.log(row_total), (block, norm_out.shape[-1]))


def attention_backward(m, full_g, w_out, kept, outs, mix_buf, acc, scale, block):
    q_in, k_in, v_in, o_in, norm_in = kept
    dq_out, dk_out, dv_out = outs
    mix_buf[...] = mm(rows_of(full_g, m), w_out[...], 1, 1).astype(B16)
    seq = mix_buf.shape[0]
    acc[...] = jnp.zeros_like(acc)
    for start in range(0, seq, block):
        stop = start + block
        queries, mix = q_in[m, start:stop], mix_buf[start:stop]
        keys = k_in[m, :stop]
        scores = causal(mm(queries, keys, 1, 1) * scale, start)
        prob = jnp.exp(scores - norm_in[m, start:stop, :1])
        grad_prob = mm(mix, v_in[m, :stop], 1, 1).astype(B16).astype(F32)
        row_dot = jnp.sum(grad_prob * prob, axis=-1, keepdims=True)
        grad_scores = (prob * (grad_prob - row_dot) * scale).astype(B16)
        dq_out[m, start:stop] = mm(grad_scores, keys, 1, 0).astype(B16)
        acc[0, :stop] += mm(grad_scores, queries, 0, 0)
        acc[1, :stop] += mm(prob.astype(B16), mix, 0, 0)
    dk_out[m] = acc[0].astype(B16)
    dv_out[m] = acc[1].astype(B16)


def mlp_forward(m, full, w_gate, w_up, out, block):
    rows = rows_of(full, m)
    for start in range(0, rows.shape[0], block):
        part = rows[start:start + block]
        gate = mm(part, w_gate[...], 1, 0)
        up = mm(part, w_up[...], 1, 0)
        out[m, start:start + block] = (gate * lax.logistic(gate) * up).astype(B16)


def mlp_backward(m, full_v, full_g, w_gate, w_up, w_down, dgate_out, dup_out, inner_buf, block):
    rows, grads = rows_of(full_v, m), rows_of(full_g, m)
    for start in range(0, rows.shape[0], block):
        part = rows[start:start + block]
        gate = mm(part, w_gate[...], 1, 0)
        up = mm(part, w_up[...], 1, 0)
        sig = lax.logistic(gate)
        act = gate * sig
        inner_buf[start:start + block] = (act * up).astype(B16)
        grad_inner = mm(grads[start:start + block], w_down[...], 1, 1).astype(B16).astype(F32)
        dup_out[m, start:start + block] = (grad_inner * act).astype(B16)
        dgate_out[m, start:start + block] = (grad_inner * up * sig * (1.0 + gate * (1.0 - sig))).astype(B16)


def weight_grad(m, left, right, acc, out, at, block):
    for start in range(0, right.shape[1], block):
        part = mm(left, right[:, start:start + block], 0, 0)
        cols = slice(start, start + block)
        if m == 0:
            acc[:, cols] = part
        else:
            total = (acc[:, cols] + part).astype(B16)
            if at is None:
                out[:, cols] = total
            else:
                out[at, :, cols] = total


def weight_grad_rows(m, left, right, acc, out, block):
    for start in range(0, left.shape[1], block):
        part = mm(left[:, start:start + block], right, 0, 0)
        if m == 0:
            acc[start:start + block] = part
        else:
            out[start:start + block] = (acc[start:start + block] + part).astype(B16)


def stage_call(side, cid, kind, post, left, right, layer, transposed, row_ins, gain, extra, grads, weights, kept, scale):
    micro, rows, width = row_ins[0].shape
    quarter = width // 4
    seq = side * side * CORES * rows
    sds = jax.ShapeDtypeStruct
    shard = sds((micro, rows, width), B16)
    part = sds((1, width), F32)
    reduces = kind != 'norm'
    new_full = kind in ('norm', 'fwd', 'bwd')
    outs = {'norm': [shard], 'fwd': [shard, shard], 'fwd_last': [shard], 'bwd': [shard, part], 'bwd_last': [shard]}[kind]
    n_small = len(outs)
    n_full = len(extra) + new_full
    total_reduce = kind == 'bwd_last'
    n_terms = len(grads) + 1
    if total_reduce:
        outs = outs + [sds((8, width), F32)]
    post_outs, post_scratch = [], []
    head = weights[0].shape[-2] if post in ('attn', 'attn_bwd') else 0
    if post == 'attn':
        post_outs = [sds((micro, seq, head), B16)] * 4 + [sds((micro, seq, 128), F32)]
    elif post == 'mlp':
        post_outs = [sds((micro, seq, weights[0].shape[-1]), B16)]
    elif post == 'attn_bwd':
        post_outs = [sds((micro, seq, head), B16)] * 3 + [sds((head, width), B16), sds((3, head, width), B16)]
        post_scratch = [pltpu.VMEM((seq, head), B16), pltpu.VMEM((2, seq, head), F32), pltpu.VMEM((head, width), F32), pltpu.VMEM((3, head, width), F32)]
    elif post == 'mlp_bwd':
        ff = weights[0].shape[-1]
        post_outs = [sds((micro, seq, ff), B16)] * 2 + [sds((width, ff), B16)] * 2 + [sds((ff, width), B16)]
        post_scratch = [pltpu.VMEM((seq, ff), B16), pltpu.VMEM((width, ff), F32), pltpu.VMEM((width, ff), F32), pltpu.VMEM((ff, width), F32)]
    outs = outs + post_outs
    scratch = [pltpu.VMEM((micro, side, side, CORES, rows, width), B16)] * n_full
    n_pair, n_weights = len(left), len(weights)
    if reduces:
        piece = (micro, 2, side, 2, side, rows, quarter)
        scratch += [pltpu.VMEM(piece, F32)] * 3
        scratch += [pltpu.VMEM((micro, 2, 6, side, rows, quarter), F32), pltpu.VMEM((micro, 2, 6, rows, quarter), F32),
                    pltpu.VMEM((micro, rows, width), F32)]
    scratch += [pltpu.VMEM(item.shape[1:], B16) for item in right + weights] + [pltpu.SemaphoreType.DMA((max(1, len(right) + n_weights),))]
    if total_reduce:
        scratch += [pltpu.VMEM((8, width), F32), pltpu.VMEM((8, width), F32), pltpu.VMEM((2, side, 8, width), F32)]
    n_sems = micro * (48 * n_full + (32 if reduces else 0)) + (7 if total_reduce else 0)
    scratch += post_scratch + [pltpu.SemaphoreType.DMA((n_sems,)), pltpu.SemaphoreType.DMA((n_sems,))]
    n_rows, n_extra, n_grads, n_right, n_kept = len(row_ins), len(extra), len(grads), len(right), len(kept)
    has_gain = gain is not None

    def body(*refs):
        refs = list(refs)

        def take(count):
            got, refs[:] = refs[:count], refs[count:]
            return got
        lefts, rights, row_refs = take(n_pair), take(n_right), take(n_rows)
        gain_ref = take(1)[0] if has_gain else None
        extra_refs, grad_refs, weight_refs, kept_refs = take(n_extra), take(n_grads), take(n_weights), take(n_kept)
        small_outs = take(n_small)
        total_out = take(1)[0] if total_reduce else None
        post_refs = take(len(post_outs))
        full_bufs = take(n_full)
        if reduces:
            send_buf, own_buf, chip_buf, ring_buf, tail_buf, sums = take(6)
        held = take(n_right + n_weights)
        weight_sems = take(1)[0]
        loads = []
        for i, ref in enumerate(rights + weight_refs):
            loads.append(pltpu.make_async_copy(ref.at[layer[0] if i < n_right else layer[1]], held[i], weight_sems.at[i]))
            loads[-1].start()
        product_weights, post_weights = held[:n_right], held[n_right:]
        if total_reduce:
            value, pair_buf, ring_bufs = take(3)
        work = take(len(post_scratch))
        send_sems, recv_sems = take(2)
        place = Place(side)
        copies = Copies(send_sems, recv_sems)
        entered = entry_barrier(place)
        for ref, out in zip(extra_refs, full_bufs):
            for m in range(micro):
                out[m, place.y, place.x, place.core] = ref[m]
        gain_parts = []

        def gather_new(m):
            gain_row = gain_ref[...] if has_gain else None
            new = None
            if kind == 'norm':
                new = rms_scale(row_refs[0][m].astype(F32), gain_row).astype(B16)
                small_outs[0][m] = new
            elif kind == 'fwd':
                small_outs[0][m], new = epilogue_forward(sums[m], row_refs[0][m], gain_row)
                small_outs[1][m] = new
            elif kind == 'fwd_last':
                small_outs[0][m] = (row_refs[0][m].astype(F32) + sums[m].astype(B16).astype(F32)).astype(B16)
            else:
                new, gain_part = epilogue_backward(sums[m], row_refs[0][m], gain_row, row_refs[1][m])
                small_outs[0][m] = new
                gain_parts.append(gain_part)
            if new_full:
                full_bufs[-1][m, place.y, place.x, place.core] = new

        def post_a(m):
            if m == 0:
                for load in loads[n_right:]:
                    load.wait()
            if post == 'attn':
                attention_forward(m, full_bufs[-1], post_weights[0], post_refs, scale, 128)
            elif post == 'mlp':
                mlp_forward(m, full_bufs[-1], post_weights[0], post_weights[1], post_refs[0], 256)
            elif post == 'attn_bwd':
                attention_backward(m, full_bufs[-1], post_weights[0], kept_refs, post_refs[:3], work[0], work[1], scale, 128)
            elif post == 'mlp_bwd':
                mlp_backward(m, full_bufs[0], full_bufs[-1], *post_weights, post_refs[0], post_refs[1], work[0], 256)

        def post_b(m):
            if post == 'attn_bwd':
                weight_grad(m, kept_refs[3][m], rows_of(full_bufs[-1], m), work[2], post_refs[3], None, 512)
                for i in range(3):
                    weight_grad(m, post_refs[i][m], rows_of(full_bufs[0], m), work[3].at[i], post_refs[4], i, 512)
            elif post == 'mlp_bwd':
                rows_v = rows_of(full_bufs[0], m)
                weight_grad_rows(m, rows_v, post_refs[0][m], work[1], post_refs[2], 512)
                weight_grad_rows(m, rows_v, post_refs[1][m], work[2], post_refs[3], 512)
                weight_grad(m, work[0][...], rows_of(full_bufs[-1], m), work[3], post_refs[4], None, 512)

        early = [AllGather(place, copies, [buf.at[m] for buf in full_bufs[:n_extra]]) for m in range(micro)]
        late = [AllGather(place, copies, [full_bufs[-1].at[m]] if new_full else []) for m in range(micro)]
        first_early = not new_full

        def early_step(name, when):
            if when == first_early:
                for job in early:
                    getattr(job, name)()
        if reduces:
            for load in loads[:n_right]:
                load.wait()
            pairs = [(a, b, transposed) for a, b in zip(lefts, [product_weights[0].at[i] for i in range(n_pair)] if n_pair > n_right else product_weights)]
            sum0, sum1 = (ReduceScatter(place, copies, pairs, m, send_buf, own_buf, chip_buf, ring_buf, tail_buf, sums)
                          for m in range(micro))
            sum0.p0(entered)
            early_step('a0', True)
            sum0.p1()
            sum0.p2()
            sum1.p0()
            sum0.p3()
            sum1.p1()
            sum1.p2()
            sum0.p4()
            sum1.p3()
            early_step('a1', True)
            sum0.p5()
            sum1.p4()
            sum0.p6()
            early_step('a2', True)
            early_step('a0', False)
            sum1.p5()
            sum0.p7()
        else:
            entered()
        gather_new(0)
        late[0].a0()
        if reduces:
            sum1.p6()
            late[0].a1()
            early_step('a1', False)
            early_step('a3', True)
            sum1.p7()
        gather_new(1)
        late[1].a0()
        if not reduces:
            late[0].a1()
        late[0].a2()
        early_step('a2', False)
        late[1].a1()
        late[0].a3()
        early_step('a3', False)
        late[1].a2()
        late[0].a4()
        late[1].a3()
        late[0].a5()
        late[1].a4()
        early[0].a4()
        late[0].a6()
        early_first = post == 'mlp_bwd'
        if not early_first:
            post_a(0)
        late[1].a5()
        early[1].a4()
        early[0].a5()
        early[0].a6()
        if early_first:
            post_a(0)
        early[1].a5()
        post_b(0)
        early[1].a6()
        late[1].a6()
        post_a(1)
        post_b(1)
        if total_reduce:
            value[...] = jnp.zeros_like(value)
            for i, ref in enumerate(grad_refs):
                value[i:i + 1] = ref[...]
            value[n_terms - 1:n_terms] = gain_parts[0] + gain_parts[1]
            all_reduce(place, copies, value, pair_buf, ring_bufs, total_out)
        elif gain_parts:
            small_outs[1][...] = gain_parts[0] + gain_parts[1]
        copies.finish()

    ins = list(left) + list(right) + list(row_ins) + ([gain.reshape(1, width)] if has_gain else []) + list(extra) + list(grads)
    vmem = pl.BlockSpec(memory_space=pltpu.VMEM)
    whole = pl.BlockSpec(memory_space=pl.ANY)
    in_specs = [vmem] * len(ins)
    in_specs[n_pair:n_pair + n_right] = [whole] * n_right
    in_specs += [whole] * n_weights + [vmem] * n_kept
    ins += list(weights) + list(kept)
    return pl.pallas_call(
        body, out_shape=outs, in_specs=in_specs, out_specs=[vmem] * len(outs), scratch_shapes=scratch,
        compiler_params=pltpu.CompilerParams(collective_id=cid, has_side_effects=True, vmem_limit_bytes=64 * 1024 * 1024 - 65536),
        name=f'stage_{kind}_{cid}')(*ins)


def solution(mesh):
    row_spec = P(None, ('dp', 'tp'), None)
    gain_spec = P(None, None)
    qkv_spec = P(None, None, 'tp', None, None)
    head_spec = P(None, 'tp', None, None)
    col_spec = P(None, None, 'tp')
    row_shard_spec = P(None, 'tp', None)
    side = math.isqrt(mesh.shape['tp'] // CORES)

    def device_program(x_in, y_cot, gain_attn, gain_mlp, w_qkv, w_out, w_gate, w_up, w_down):
        micro, rows, width = x_in.shape
        layer_count = w_qkv.shape[0]
        slots = w_qkv.shape[2] * w_qkv.shape[3]
        head_dim = w_qkv.shape[4]
        assert slots == 3 and side == 4 and micro == 2
        qkv_flat = w_qkv.transpose(0, 2, 3, 4, 1).reshape(layer_count, slots, head_dim, width)
        out_flat = w_out.reshape(layer_count, head_dim, width)
        call_ids = iter(range(64))

        def stage(kind, post=None, left=(), right=(), layer=(0, 0), transposed=False, row_ins=(), gain=None, extra=(), grads=(), weights=(), kept=()):
            left = [item.reshape(micro, side * side, CORES, rows, item.shape[-1]) for item in left]
            return stage_call(side, next(call_ids), kind, post, left, list(right), layer, transposed, list(row_ins), gain, list(extra),
                              list(grads), list(weights), list(kept), head_dim ** -0.5)

        kept = []
        rows_x = x_in
        normed, *attn = stage('norm', 'attn', layer=(0, 0), row_ins=[x_in], gain=gain_attn[0], weights=[qkv_flat])
        for layer in range(layer_count):
            hidden, normed_b, inner = stage('fwd', 'mlp', [attn[3]], [out_flat], (layer, layer), False, [rows_x], gain_mlp[layer],
                                            weights=[w_gate, w_up])
            kept.append((rows_x, normed, hidden, normed_b, attn))
            if layer + 1 < layer_count:
                rows_x, normed, *attn = stage('fwd', 'attn', [inner], [w_down], (layer, layer + 1), False, [hidden], gain_attn[layer + 1],
                                              weights=[qkv_flat])
            else:
                rows_y, *mlp = stage('fwd_last', 'mlp_bwd', [inner], [w_down], (layer, layer), False, [hidden], None, [normed_b, y_cot],
                                     weights=[w_gate, w_up, w_down])

        grad_rows = y_cot
        out_grads = [[None] * layer_count for _ in range(5)]
        gain_parts = {}
        for layer in reversed(range(layer_count)):
            rows_x, normed, hidden, normed_b, attn = kept[layer]
            grad_gate, grad_up, out_grads[2][layer], out_grads[3][layer], out_grads[4][layer] = mlp
            grad_hidden, gain_parts['mlp', layer], *grad_qkv, out_grads[1][layer], out_grads[0][layer] = stage(
                'bwd', 'attn_bwd', [grad_gate, grad_up], [w_gate, w_up], (layer, layer), True, [hidden, grad_rows], gain_mlp[layer], [normed],
                weights=[out_flat], kept=attn)
            if layer > 0:
                grad_rows, gain_parts['attn', layer], *mlp = stage(
                    'bwd', 'mlp_bwd', grad_qkv, [qkv_flat], (layer, layer - 1), False, [rows_x, grad_hidden], gain_attn[layer], [kept[layer - 1][3]],
                    weights=[w_gate, w_up, w_down])
            else:
                terms = [gain_parts['attn', item] for item in range(1, layer_count)] + [gain_parts['mlp', item] for item in range(layer_count)]
                grad_rows, gain_sums = stage(
                    'bwd_last', None, grad_qkv, [qkv_flat], (layer, layer), False, [rows_x, grad_hidden], gain_attn[layer], grads=terms)
        n_attn = layer_count - 1
        gain_a = jnp.concatenate([gain_sums[2 * layer_count - 1:2 * layer_count], gain_sums[:n_attn]], axis=0)
        gain_b = gain_sums[n_attn:n_attn + layer_count]
        return (rows_y, grad_rows,
                jnp.stack(out_grads[0]).reshape(layer_count, 1, slots, head_dim, width).transpose(0, 4, 1, 2, 3), jnp.stack(out_grads[1]).reshape(w_out.shape),
                jnp.stack(out_grads[2]), jnp.stack(out_grads[3]), jnp.stack(out_grads[4]), gain_a, gain_b)

    return jax.shard_map(device_program, mesh=mesh,
                         in_specs=(row_spec, row_spec, gain_spec, gain_spec, qkv_spec, head_spec, col_spec, col_spec, row_shard_spec),
                         out_specs=(row_spec, row_spec, P('dp', None, 'tp', None, None), P('dp', 'tp', None, None), P('dp', None, 'tp'), P('dp', None, 'tp'), P('dp', 'tp', None), P('dp', None), P('dp', None)),
                         check_vma=False)
```

```python
import functools
import math

import jax
import jax.numpy as jnp
from jax import lax
from jax.experimental import pallas as pl
from jax.experimental.pallas import tpu as pltpu
from jax.sharding import PartitionSpec as P

NORM_EPS = 1e-5
MESH = pl.DeviceIdType.MESH
CORES = 2
F32 = jnp.float32
B16 = jnp.bfloat16


def rms_scale(row_vals, gain_vec):
    return row_vals * lax.rsqrt(jnp.mean(row_vals * row_vals, axis=-1, keepdims=True) + NORM_EPS) * gain_vec


class Place:
    def __init__(self, side):
        me = lax.axis_index('tp')
        self.side = side
        self.core = lax.rem(me, CORES)
        chip = lax.div(me, CORES)
        self.x = lax.rem(chip, side)
        self.y = lax.div(chip, side)
        self.partner = self.dev(self.y, self.x, 1 - self.core)

    def dev(self, y, x, core):
        return {'tp': (y * self.side + x) * CORES + core}

    def shift(self, coord, by):
        return lax.rem(coord + by + self.side, self.side)

    def on_ring(self, axis, by):
        if axis == 0:
            return self.dev(self.y, self.shift(self.x, by), self.core)
        return self.dev(self.shift(self.y, by), self.x, self.core)


class Copies:
    def __init__(self, send_sems, recv_sems):
        self.send_sems = send_sems
        self.recv_sems = recv_sems
        self.send_groups, self.recv_groups = {}, {}
        self.recv_count = 0

    def start(self, src, dst, target, group, total, recv_group=None):
        if group not in self.send_groups:
            self.send_groups[group] = (len(self.send_groups), total)
        if recv_group is None:
            recv_idx = self.recv_count
            self.recv_count += 1
        else:
            if recv_group not in self.recv_groups:
                self.recv_groups[recv_group] = self.recv_count
                self.recv_count += 1
            recv_idx = self.recv_groups[recv_group]
        copy = pltpu.make_async_remote_copy(src_ref=src, dst_ref=dst, send_sem=self.send_sems.at[self.send_groups[group][0]],
                                            recv_sem=self.recv_sems.at[recv_idx], device_id=target, device_id_type=MESH)
        copy.start()
        return copy

    def wait_group(self, recv_group, total):
        pltpu.make_async_copy(total, total, self.recv_sems.at[self.recv_groups[recv_group]]).wait()

    def finish(self):
        for idx, total in self.send_groups.values():
            pltpu.make_async_copy(total, total, self.send_sems.at[idx]).wait()


def entry_barrier(place):
    targets = [place.partner] + [place.on_ring(axis, by) for axis in (0, 1) for by in (1, -1, 2)]
    barrier = pltpu.get_barrier_semaphore()
    for target in targets:
        pl.semaphore_signal(barrier, inc=1, device_id=target, device_id_type=MESH)
    return lambda: pl.semaphore_wait(barrier, len(targets))


def add_rows(dst, *terms):
    def body(i, carry):
        total = terms[0][i]
        for term in terms[1:]:
            total = total + term[i]
        dst[i] = total
        return carry
    lax.fori_loop(0, dst.shape[0], body, 0)


class ReduceScatter:
    def __init__(self, place, copies, pairs, m, send_buf, own_buf, chip_buf, ring_buf, tail_buf, sums):
        self.place, self.copies, self.pairs, self.m = place, copies, pairs, m
        self.send_buf, self.own_buf, self.chip_buf, self.ring_buf, self.tail_buf, self.sums = (
            ref.at[m] for ref in (send_buf, own_buf, chip_buf, ring_buf, tail_buf, sums))
        self.quarter = self.own_buf.shape[-1]
        self.rows = self.own_buf.shape[-2]
        self.spots = [(coord, place.shift(coord, 1), place.shift(coord, -1), place.shift(coord, 2))
                      for coord in (place.x, place.y)]
        self.chip_copies, self.first, self.second = {}, {}, {}

    def products(self, half, core, buf):
        side, rows, quarter = self.place.side, self.rows, self.quarter

        def one(sub, carry):
            cols = pl.ds(pl.multiple_of((half * 2 + sub) * quarter, quarter), quarter)
            total = None
            for a_ref, b_ref, transposed in self.pairs:
                left = a_ref[self.m, :, core].reshape(side * side * rows, a_ref.shape[-1])
                if transposed:
                    part = lax.dot_general(left, b_ref[cols, :], (((1,), (1,)), ((), ())), preferred_element_type=F32)
                else:
                    part = jnp.dot(left, b_ref[:, cols], preferred_element_type=F32)
                total = part if total is None else total + part
            total = total.reshape(side, side, rows, quarter)
            for yy in range(side):
                for xx in range(side):
                    first, second = (xx, yy) if half == 0 else (yy, xx)
                    buf[half, first, sub, second] = total[yy, xx]
            return carry
        lax.fori_loop(0, 2, one, 0)

    def p0(self, entered=None):
        for half in (0, 1):
            self.products(half, 1 - self.place.core, self.send_buf)
            if entered is not None and half == 0:
                entered()
            self.to_partner(half, 'far', self.spots[half][3])
        for half in (0, 1):
            here, plus, minus, far = self.spots[half]
            for name, spot in (('plus', plus), ('minus', minus), ('here', here)):
                self.to_partner(half, name, spot)

    def to_partner(self, half, name, spot):
        self.chip_copies[half, name] = self.copies.start(self.send_buf.at[half, spot], self.chip_buf.at[half, spot], self.place.partner,
                                                              ('chip', self.m), self.send_buf)

    def p1(self):
        for half in (0, 1):
            self.products(half, self.place.core, self.own_buf)

    def join(self, half, name, spot):
        self.chip_copies[half, name].wait_recv()
        for sub in (0, 1):
            add_rows(self.own_buf.at[half, spot, sub], self.own_buf.at[half, spot, sub], self.chip_buf.at[half, spot, sub])

    def ring(self, half, slot, spot, sub, by):
        self.first[half, slot] = self.copies.start(self.own_buf.at[half, spot, sub], self.ring_buf.at[half, slot], self.place.on_ring(half, by),
                                                    ('ring', self.m), self.ring_buf)

    def tail(self, half, slot, spot, sub, by):
        here = self.spots[half][0]
        self.second[half, slot] = self.copies.start(self.own_buf.at[half, here, sub, spot], self.tail_buf.at[half, slot],
                                                    self.place.on_ring(1 - half, by), ('tail', self.m), self.tail_buf)

    def p2(self):
        for half in (0, 1):
            far = self.spots[half][3]
            self.join(half, 'far', far)
            self.ring(half, 0, far, 0, 1)
            self.ring(half, 1, far, 1, -1)

    def p3(self):
        for half in (0, 1):
            here, plus, minus, far = self.spots[half]
            self.join(half, 'plus', plus)
            self.ring(half, 2, plus, 1, 1)
            self.join(half, 'minus', minus)
            self.ring(half, 3, minus, 0, -1)
        for half in (0, 1):
            self.join(half, 'here', self.spots[half][0])

    def p4(self):
        own, ring = self.own_buf, self.ring_buf
        for half in (0, 1):
            here, plus, minus, far = self.spots[half]
            self.first[half, 0].wait_recv()
            add_rows(own.at[half, plus, 0], own.at[half, plus, 0], ring.at[half, 0])
            self.ring(half, 4, plus, 0, 1)
            self.first[half, 1].wait_recv()
            add_rows(own.at[half, minus, 1], own.at[half, minus, 1], ring.at[half, 1])
            self.ring(half, 5, minus, 1, -1)

    def p5(self):
        own, ring = self.own_buf, self.ring_buf
        for half in (0, 1):
            here = self.spots[half][0]
            _, plus, minus, far = self.spots[1 - half]
            for slot in (2, 3, 4, 5):
                self.first[half, slot].wait_recv()
            add_rows(own.at[half, here, 0], own.at[half, here, 0], ring.at[half, 3], ring.at[half, 4])
            add_rows(own.at[half, here, 1], own.at[half, here, 1], ring.at[half, 2], ring.at[half, 5])
            self.tail(half, 0, far, 0, 1)
            self.tail(half, 1, far, 1, -1)
            self.tail(half, 2, plus, 1, 1)
            self.tail(half, 3, minus, 0, -1)

    def p6(self):
        own, tail = self.own_buf, self.tail_buf
        for half in (0, 1):
            here = self.spots[half][0]
            _, plus, minus, _ = self.spots[1 - half]
            self.second[half, 0].wait_recv()
            own[half, here, 0, plus] = own[half, here, 0, plus] + tail[half, 0]
            self.tail(half, 4, plus, 0, 1)
            self.second[half, 1].wait_recv()
            own[half, here, 1, minus] = own[half, here, 1, minus] + tail[half, 1]
            self.tail(half, 5, minus, 1, -1)

    def p7(self):
        own, tail, quarter = self.own_buf, self.tail_buf, self.quarter
        for half in (0, 1):
            here, mine = self.spots[half][0], self.spots[1 - half][0]
            for slot in (2, 3, 4, 5):
                self.second[half, slot].wait_recv()
            start = half * 2 * quarter
            self.sums[:, start:start + quarter] = own[half, here, 0, mine] + tail[half, 3] + tail[half, 4]
            self.sums[:, start + quarter:start + 2 * quarter] = own[half, here, 1, mine] + tail[half, 2] + tail[half, 5]


class AllGather:
    def __init__(self, place, copies, arrays, tag):
        self.place, self.copies, self.tag = place, copies, tag
        self.arrays = arrays
        self.coords = (place.x, place.y)
        self.jobs = [(array, half, i) for i, array in enumerate(arrays) for half in (0, 1)]
        self.first, self.second = {}, {}

    def send(self, job, spot, other, sub, axis, by, kind):
        array, half, i = job
        total = {'first': array.at[0, 0:3, 0], 'second': array.at[0], 'sub': array.at[0, 0:2]}[kind]
        yy, xx = (other, spot) if half == 0 else (spot, other)
        half_cols = array.shape[-1] // 2
        cols = pl.ds(half * half_cols, half_cols) if sub is None else pl.ds(half * half_cols + sub * half_cols // 2, half_cols // 2)
        ref = array.at[yy, xx, self.place.core, :, cols]
        return self.copies.start(ref, ref, self.place.on_ring(axis, by), (kind, self.tag, i), total,
                                 (kind, self.tag, i) if kind == 'sub' else None)

    def send_line(self, job, other):
        array, half, i = job
        half_cols = array.shape[-1] // 2
        cols = pl.ds(half * half_cols, half_cols)
        core = self.place.core
        ref = array.at[other, :, core, :, cols] if half == 0 else array.at[:, other, core, :, cols]
        self.copies.start(ref, ref, self.place.partner, ('line', self.tag, i), array.at[0:2], ('line', self.tag, i))

    def each(self):
        for j, job in enumerate(self.jobs):
            half = job[1]
            yield j, job, half, self.coords[half], self.coords[1 - half]

    def a0(self):
        for j, job, half, spot, other in self.each():
            for by in (1, -1, 2):
                self.first[j, by] = self.send(job, spot, other, None, half, by, 'first')
            for by in (1, -1):
                self.second[j, 0, by] = self.send(job, spot, other, None, 1 - half, by, 'second')

    def a1(self):
        for j, job, half, spot, other in self.each():
            for by in (1, -1):
                self.first[j, by].wait_recv()
                came = self.place.shift(spot, -by)
                for to in (1, -1):
                    self.second[j, -by, to] = self.send(job, came, other, None, 1 - half, to, 'second')

    def a2(self):
        for j, job, half, spot, other in self.each():
            self.first[j, 2].wait_recv()
            far = self.place.shift(spot, 2)
            for to in (1, -1):
                self.second[j, 2, to] = self.send(job, far, other, None, 1 - half, to, 'second')
            self.send_line(job, other)

    def a3(self):
        for off in (0, 1, -1):
            self.pass_on(off)

    def pass_on(self, off):
        for j, job, half, spot, other in self.each():
            for to, sub in ((1, 0), (-1, 1)):
                self.second[j, off, to].wait_recv()
                came = self.place.shift(other, -to)
                self.send(job, self.place.shift(spot, off), came, sub, 1 - half, to, 'sub')

    def a4(self):
        self.pass_on(2)
        for j, job, half, spot, other in self.each():
            for to in (1, -1):
                self.send_line(job, self.place.shift(other, to))

    def a5(self):
        for i, array in enumerate(self.arrays):
            self.copies.wait_group(('sub', self.tag, i), array.at[0, 0:2])
        for j, job, half, spot, other in self.each():
            self.send_line(job, self.place.shift(other, 2))

    def a6(self):
        for i, array in enumerate(self.arrays):
            self.copies.wait_group(('line', self.tag, i), array.at[0:2])


def all_reduce(place, copies, value, pair_buf, ring_bufs, out):
    side = place.side
    copy = copies.start(value, pair_buf, place.partner, 'pair', value)
    copy.wait_recv()
    total = value[...] + pair_buf[...]
    for axis in (0, 1):
        coord = place.x if axis == 0 else place.y
        buf = ring_bufs.at[axis]
        buf[coord] = total
        going = [copies.start(buf.at[coord], buf.at[coord], place.on_ring(axis, by), ('all', axis), buf.at[0:3]) for by in (1, -1, 2)]
        for copy in going:
            copy.wait_recv()
        total = buf[0]
        for k in range(1, side):
            total = total + buf[k]
    out[...] = total


def epilogue_forward(sums, residual, gain):
    new_rows = (residual.astype(F32) + sums.astype(B16).astype(F32)).astype(B16)
    return new_rows, rms_scale(new_rows.astype(F32), gain).astype(B16)


def epilogue_backward(sums, rows_in, gain, cot):
    vals = rows_in.astype(F32)
    grad = sums.astype(B16).astype(F32)
    inv = lax.rsqrt(jnp.mean(vals * vals, axis=-1, keepdims=True) + NORM_EPS)
    unit = vals * inv
    scaled = grad * gain
    back = inv * (scaled - unit * jnp.mean(scaled * unit, axis=-1, keepdims=True))
    new_cot = (cot.astype(F32) + back).astype(B16)
    return new_cot, jnp.sum(grad * unit, axis=0, keepdims=True)


def mm(a, b, ca, cb):
    return lax.dot_general(a, b, (((ca,), (cb,)), ((), ())), preferred_element_type=F32)


def rows_of(full, m):
    got = full[m]
    return got.reshape(-1, got.shape[-1])


def causal(scores, start):
    row = lax.broadcasted_iota(jnp.int32, scores.shape, 0) + start
    col = lax.broadcasted_iota(jnp.int32, scores.shape, 1)
    return jnp.where(row >= col, scores, -1e30)


def attention_forward(m, full, w_qkv, outs, scale, block):
    q_out, k_out, v_out, o_out, norm_out = outs
    rows = rows_of(full, m)
    for i, out in enumerate((q_out, k_out, v_out)):
        out[m] = mm(rows, w_qkv[i], 1, 1).astype(B16)
    for start in range(0, rows.shape[0], block):
        stop = start + block
        scores = causal(mm(q_out[m, start:stop], k_out[m, :stop], 1, 1) * scale, start)
        row_max = jnp.max(scores, axis=-1, keepdims=True)
        exp_scores = jnp.exp(scores - row_max)
        row_total = jnp.sum(exp_scores, axis=-1, keepdims=True)
        prob = (exp_scores / row_total).astype(B16)
        o_out[m, start:stop] = mm(prob, v_out[m, :stop], 1, 0).astype(B16)
        norm_out[m, start:stop] = jnp.broadcast_to(row_max + jnp.log(row_total), (block, norm_out.shape[-1]))


def attention_backward(m, full_g, w_out, kept, outs, mix_buf, acc, scale, block):
    q_in, k_in, v_in, o_in, norm_in = kept
    dq_out, dk_out, dv_out = outs
    mix_buf[...] = mm(rows_of(full_g, m), w_out[...], 1, 1).astype(B16)
    seq = mix_buf.shape[0]
    acc[...] = jnp.zeros_like(acc)
    for start in range(0, seq, block):
        stop = start + block
        queries, mix = q_in[m, start:stop], mix_buf[start:stop]
        keys = k_in[m, :stop]
        scores = causal(mm(queries, keys, 1, 1) * scale, start)
        prob = jnp.exp(scores - norm_in[m, start:stop, :1])
        grad_prob = mm(mix, v_in[m, :stop], 1, 1).astype(B16).astype(F32)
        row_dot = jnp.sum(grad_prob * prob, axis=-1, keepdims=True)
        grad_scores = (prob * (grad_prob - row_dot) * scale).astype(B16)
        dq_out[m, start:stop] = mm(grad_scores, keys, 1, 0).astype(B16)
        acc[0, :stop] += mm(grad_scores, queries, 0, 0)
        acc[1, :stop] += mm(prob.astype(B16), mix, 0, 0)
    dk_out[m] = acc[0].astype(B16)
    dv_out[m] = acc[1].astype(B16)


def mlp_forward(m, full, w_gate, w_up, out, block):
    rows = rows_of(full, m)
    for start in range(0, rows.shape[0], block):
        part = rows[start:start + block]
        gate = mm(part, w_gate[...], 1, 0)
        up = mm(part, w_up[...], 1, 0)
        out[m, start:start + block] = (gate * lax.logistic(gate) * up).astype(B16)


def mlp_backward(m, full_v, full_g, w_gate, w_up, w_down, dgate_out, dup_out, inner_buf, block):
    rows, grads = rows_of(full_v, m), rows_of(full_g, m)
    for start in range(0, rows.shape[0], block):
        part = rows[start:start + block]
        gate = mm(part, w_gate[...], 1, 0)
        up = mm(part, w_up[...], 1, 0)
        sig = lax.logistic(gate)
        act = gate * sig
        inner_buf[start:start + block] = (act * up).astype(B16)
        grad_inner = mm(grads[start:start + block], w_down[...], 1, 1).astype(B16).astype(F32)
        dup_out[m, start:start + block] = (grad_inner * act).astype(B16)
        dgate_out[m, start:start + block] = (grad_inner * up * sig * (1.0 + gate * (1.0 - sig))).astype(B16)


def weight_grad(m, left, right, acc, out, at, block):
    for start in range(0, right.shape[1], block):
        part = mm(left, right[:, start:start + block], 0, 0)
        cols = slice(start, start + block)
        if m == 0:
            acc[:, cols] = part
        else:
            total = (acc[:, cols] + part).astype(B16)
            if at is None:
                out[:, cols] = total
            else:
                out[at, :, cols] = total


def weight_grad_rows(m, left, right, acc, out, block):
    for start in range(0, left.shape[1], block):
        part = mm(left[:, start:start + block], right, 0, 0)
        if m == 0:
            acc[start:start + block] = part
        else:
            out[start:start + block] = (acc[start:start + block] + part).astype(B16)


def stage_call(side, cid, kind, post, left, right, layer, transposed, row_ins, gain, extra, grads, weights, kept, scale):
    micro, rows, width = row_ins[0].shape
    quarter = width // 4
    seq = side * side * CORES * rows
    sds = jax.ShapeDtypeStruct
    shard = sds((micro, rows, width), B16)
    part = sds((1, width), F32)
    reduces = kind != 'norm'
    new_full = kind in ('norm', 'fwd', 'bwd')
    outs = {'norm': [shard], 'fwd': [shard, shard], 'fwd_last': [shard], 'bwd': [shard, part], 'bwd_last': [shard]}[kind]
    n_small = len(outs)
    n_full = len(extra) + new_full
    total_reduce = kind == 'bwd_last'
    n_terms = len(grads) + 1
    if total_reduce:
        outs = outs + [sds((8, width), F32)]
    post_outs, post_scratch = [], []
    head = weights[0].shape[-2] if post in ('attn', 'attn_bwd') else 0
    if post == 'attn':
        post_outs = [sds((micro, seq, head), B16)] * 4 + [sds((micro, seq, 128), F32)]
    elif post == 'mlp':
        post_outs = [sds((micro, seq, weights[0].shape[-1]), B16)]
    elif post == 'attn_bwd':
        post_outs = [sds((micro, seq, head), B16)] * 3 + [sds((head, width), B16), sds((3, head, width), B16)]
        post_scratch = [pltpu.VMEM((seq, head), B16), pltpu.VMEM((2, seq, head), F32), pltpu.VMEM((head, width), F32), pltpu.VMEM((3, head, width), F32)]
    elif post == 'mlp_bwd':
        ff = weights[0].shape[-1]
        post_outs = [sds((micro, seq, ff), B16)] * 2 + [sds((width, ff), B16)] * 2 + [sds((ff, width), B16)]
        post_scratch = [pltpu.VMEM((seq, ff), B16), pltpu.VMEM((width, ff), F32), pltpu.VMEM((width, ff), F32), pltpu.VMEM((ff, width), F32)]
    outs = outs + post_outs
    scratch = [pltpu.VMEM((micro, side, side, CORES, rows, width), B16)] * n_full
    n_pair, n_weights = len(left), len(weights)
    if reduces:
        piece = (micro, 2, side, 2, side, rows, quarter)
        scratch += [pltpu.VMEM(piece, F32)] * 3
        scratch += [pltpu.VMEM((micro, 2, 6, side, rows, quarter), F32), pltpu.VMEM((micro, 2, 6, rows, quarter), F32),
                    pltpu.VMEM((micro, rows, width), F32)]
    scratch += [pltpu.VMEM(item.shape[1:], B16) for item in right + weights] + [pltpu.SemaphoreType.DMA((max(1, len(right) + n_weights),))]
    if total_reduce:
        scratch += [pltpu.VMEM((8, width), F32), pltpu.VMEM((8, width), F32), pltpu.VMEM((2, side, 8, width), F32)]
    n_send = micro * (4 * n_full + (3 if reduces else 0)) + (3 if total_reduce else 0)
    n_recv = micro * (24 * n_full + (32 if reduces else 0)) + (7 if total_reduce else 0)
    scratch += post_scratch + [pltpu.SemaphoreType.DMA((n_send,)), pltpu.SemaphoreType.DMA((n_recv,))]
    n_rows, n_extra, n_grads, n_right, n_kept = len(row_ins), len(extra), len(grads), len(right), len(kept)
    has_gain = gain is not None

    def body(*refs):
        refs = list(refs)

        def take(count):
            got, refs[:] = refs[:count], refs[count:]
            return got
        lefts, rights, row_refs = take(n_pair), take(n_right), take(n_rows)
        gain_ref = take(1)[0] if has_gain else None
        extra_refs, grad_refs, weight_refs, kept_refs = take(n_extra), take(n_grads), take(n_weights), take(n_kept)
        small_outs = take(n_small)
        total_out = take(1)[0] if total_reduce else None
        post_refs = take(len(post_outs))
        full_bufs = take(n_full)
        if reduces:
            send_buf, own_buf, chip_buf, ring_buf, tail_buf, sums = take(6)
        held = take(n_right + n_weights)
        weight_sems = take(1)[0]
        loads = []
        for i, ref in enumerate(rights + weight_refs):
            loads.append(pltpu.make_async_copy(ref.at[layer[0] if i < n_right else layer[1]], held[i], weight_sems.at[i]))
            loads[-1].start()
        product_weights, post_weights = held[:n_right], held[n_right:]
        if total_reduce:
            value, pair_buf, ring_bufs = take(3)
        work = take(len(post_scratch))
        send_sems, recv_sems = take(2)
        place = Place(side)
        copies = Copies(send_sems, recv_sems)
        entered = entry_barrier(place)
        for ref, out in zip(extra_refs, full_bufs):
            for m in range(micro):
                out[m, place.y, place.x, place.core] = ref[m]
        gain_parts = []

        def gather_new(m):
            gain_row = gain_ref[...] if has_gain else None
            new = None
            if kind == 'norm':
                new = rms_scale(row_refs[0][m].astype(F32), gain_row).astype(B16)
                small_outs[0][m] = new
            elif kind == 'fwd':
                small_outs[0][m], new = epilogue_forward(sums[m], row_refs[0][m], gain_row)
                small_outs[1][m] = new
            elif kind == 'fwd_last':
                small_outs[0][m] = (row_refs[0][m].astype(F32) + sums[m].astype(B16).astype(F32)).astype(B16)
            else:
                new, gain_part = epilogue_backward(sums[m], row_refs[0][m], gain_row, row_refs[1][m])
                small_outs[0][m] = new
                gain_parts.append(gain_part)
            if new_full:
                full_bufs[-1][m, place.y, place.x, place.core] = new

        def post_a(m):
            if m == 0:
                for load in loads[n_right:]:
                    load.wait()
            if post == 'attn':
                attention_forward(m, full_bufs[-1], post_weights[0], post_refs, scale, 128)
            elif post == 'mlp':
                mlp_forward(m, full_bufs[-1], post_weights[0], post_weights[1], post_refs[0], 256)
            elif post == 'attn_bwd':
                attention_backward(m, full_bufs[-1], post_weights[0], kept_refs, post_refs[:3], work[0], work[1], scale, 128)
            elif post == 'mlp_bwd':
                mlp_backward(m, full_bufs[0], full_bufs[-1], *post_weights, post_refs[0], post_refs[1], work[0], 256)

        def post_b(m):
            if post == 'attn_bwd':
                weight_grad(m, kept_refs[3][m], rows_of(full_bufs[-1], m), work[2], post_refs[3], None, 512)
                for i in range(3):
                    weight_grad(m, post_refs[i][m], rows_of(full_bufs[0], m), work[3].at[i], post_refs[4], i, 512)
            elif post == 'mlp_bwd':
                rows_v = rows_of(full_bufs[0], m)
                weight_grad_rows(m, rows_v, post_refs[0][m], work[1], post_refs[2], 512)
                weight_grad_rows(m, rows_v, post_refs[1][m], work[2], post_refs[3], 512)
                weight_grad(m, work[0][...], rows_of(full_bufs[-1], m), work[3], post_refs[4], None, 512)

        early = [AllGather(place, copies, [buf.at[m] for buf in full_bufs[:n_extra]], ('early', m)) for m in range(micro)]
        late = [AllGather(place, copies, [full_bufs[-1].at[m]] if new_full else [], ('late', m)) for m in range(micro)]
        first_early = not new_full

        def early_step(name, when):
            if when == first_early:
                for job in early:
                    getattr(job, name)()
        if reduces:
            for load in loads[:n_right]:
                load.wait()
            pairs = [(a, b, transposed) for a, b in zip(lefts, [product_weights[0].at[i] for i in range(n_pair)] if n_pair > n_right else product_weights)]
            sum0, sum1 = (ReduceScatter(place, copies, pairs, m, send_buf, own_buf, chip_buf, ring_buf, tail_buf, sums)
                          for m in range(micro))
            sum0.p0(entered)
            early_step('a0', True)
            sum0.p1()
            sum0.p2()
            sum1.p0()
            sum0.p3()
            sum1.p1()
            sum1.p2()
            sum0.p4()
            sum1.p3()
            early_step('a1', True)
            sum0.p5()
            sum1.p4()
            sum0.p6()
            early_step('a2', True)
            early_step('a0', False)
            sum1.p5()
            sum0.p7()
        else:
            entered()
        gather_new(0)
        late[0].a0()
        if reduces:
            sum1.p6()
            late[0].a1()
            early_step('a1', False)
            early_step('a3', True)
            sum1.p7()
        gather_new(1)
        late[1].a0()
        if not reduces:
            late[0].a1()
        late[0].a2()
        early_step('a2', False)
        late[1].a1()
        late[0].a3()
        early_step('a3', False)
        late[1].a2()
        late[0].a4()
        late[1].a3()
        late[0].a5()
        late[1].a4()
        early[0].a4()
        late[0].a6()
        early_first = post == 'mlp_bwd'
        if not early_first:
            post_a(0)
        late[1].a5()
        early[1].a4()
        early[0].a5()
        early[0].a6()
        if early_first:
            post_a(0)
        early[1].a5()
        post_b(0)
        early[1].a6()
        late[1].a6()
        post_a(1)
        post_b(1)
        if total_reduce:
            value[...] = jnp.zeros_like(value)
            for i, ref in enumerate(grad_refs):
                value[i:i + 1] = ref[...]
            value[n_terms - 1:n_terms] = gain_parts[0] + gain_parts[1]
            all_reduce(place, copies, value, pair_buf, ring_bufs, total_out)
        elif gain_parts:
            small_outs[1][...] = gain_parts[0] + gain_parts[1]
        copies.finish()

    ins = list(left) + list(right) + list(row_ins) + ([gain.reshape(1, width)] if has_gain else []) + list(extra) + list(grads)
    vmem = pl.BlockSpec(memory_space=pltpu.VMEM)
    whole = pl.BlockSpec(memory_space=pl.ANY)
    in_specs = [vmem] * len(ins)
    in_specs[n_pair:n_pair + n_right] = [whole] * n_right
    in_specs += [whole] * n_weights + [vmem] * n_kept
    ins += list(weights) + list(kept)
    return pl.pallas_call(
        body, out_shape=outs, in_specs=in_specs, out_specs=[vmem] * len(outs), scratch_shapes=scratch,
        compiler_params=pltpu.CompilerParams(collective_id=cid, has_side_effects=True, vmem_limit_bytes=64 * 1024 * 1024 - 65536),
        name=f'stage_{kind}_{cid}')(*ins)


def solution(mesh):
    row_spec = P(None, ('dp', 'tp'), None)
    gain_spec = P(None, None)
    qkv_spec = P(None, None, 'tp', None, None)
    head_spec = P(None, 'tp', None, None)
    col_spec = P(None, None, 'tp')
    row_shard_spec = P(None, 'tp', None)
    side = math.isqrt(mesh.shape['tp'] // CORES)

    def device_program(x_in, y_cot, gain_attn, gain_mlp, w_qkv, w_out, w_gate, w_up, w_down):
        micro, rows, width = x_in.shape
        layer_count = w_qkv.shape[0]
        slots = w_qkv.shape[2] * w_qkv.shape[3]
        head_dim = w_qkv.shape[4]
        assert slots == 3 and side == 4 and micro == 2
        qkv_flat = w_qkv.transpose(0, 2, 3, 4, 1).reshape(layer_count, slots, head_dim, width)
        out_flat = w_out.reshape(layer_count, head_dim, width)
        call_ids = iter(range(64))

        def stage(kind, post=None, left=(), right=(), layer=(0, 0), transposed=False, row_ins=(), gain=None, extra=(), grads=(), weights=(), kept=()):
            left = [item.reshape(micro, side * side, CORES, rows, item.shape[-1]) for item in left]
            return stage_call(side, next(call_ids), kind, post, left, list(right), layer, transposed, list(row_ins), gain, list(extra),
                              list(grads), list(weights), list(kept), head_dim ** -0.5)

        kept = []
        rows_x = x_in
        normed, *attn = stage('norm', 'attn', layer=(0, 0), row_ins=[x_in], gain=gain_attn[0], weights=[qkv_flat])
        for layer in range(layer_count):
            hidden, normed_b, inner = stage('fwd', 'mlp', [attn[3]], [out_flat], (layer, layer), False, [rows_x], gain_mlp[layer],
                                            weights=[w_gate, w_up])
            kept.append((rows_x, normed, hidden, normed_b, attn))
            if layer + 1 < layer_count:
                rows_x, normed, *attn = stage('fwd', 'attn', [inner], [w_down], (layer, layer + 1), False, [hidden], gain_attn[layer + 1],
                                              weights=[qkv_flat])
            else:
                rows_y, *mlp = stage('fwd_last', 'mlp_bwd', [inner], [w_down], (layer, layer), False, [hidden], None, [normed_b, y_cot],
                                     weights=[w_gate, w_up, w_down])

        grad_rows = y_cot
        out_grads = [[None] * layer_count for _ in range(5)]
        gain_parts = {}
        for layer in reversed(range(layer_count)):
            rows_x, normed, hidden, normed_b, attn = kept[layer]
            grad_gate, grad_up, out_grads[2][layer], out_grads[3][layer], out_grads[4][layer] = mlp
            grad_hidden, gain_parts['mlp', layer], *grad_qkv, out_grads[1][layer], out_grads[0][layer] = stage(
                'bwd', 'attn_bwd', [grad_gate, grad_up], [w_gate, w_up], (layer, layer), True, [hidden, grad_rows], gain_mlp[layer], [normed],
                weights=[out_flat], kept=attn)
            if layer > 0:
                grad_rows, gain_parts['attn', layer], *mlp = stage(
                    'bwd', 'mlp_bwd', grad_qkv, [qkv_flat], (layer, layer - 1), False, [rows_x, grad_hidden], gain_attn[layer], [kept[layer - 1][3]],
                    weights=[w_gate, w_up, w_down])
            else:
                terms = [gain_parts['attn', item] for item in range(1, layer_count)] + [gain_parts['mlp', item] for item in range(layer_count)]
                grad_rows, gain_sums = stage(
                    'bwd_last', None, grad_qkv, [qkv_flat], (layer, layer), False, [rows_x, grad_hidden], gain_attn[layer], grads=terms)
        n_attn = layer_count - 1
        gain_a = jnp.concatenate([gain_sums[2 * layer_count - 1:2 * layer_count], gain_sums[:n_attn]], axis=0)
        gain_b = gain_sums[n_attn:n_attn + layer_count]
        return (rows_y, grad_rows,
                jnp.stack(out_grads[0]).reshape(layer_count, 1, slots, head_dim, width).transpose(0, 4, 1, 2, 3), jnp.stack(out_grads[1]).reshape(w_out.shape),
                jnp.stack(out_grads[2]), jnp.stack(out_grads[3]), jnp.stack(out_grads[4]), gain_a, gain_b)

    return jax.shard_map(device_program, mesh=mesh,
                         in_specs=(row_spec, row_spec, gain_spec, gain_spec, qkv_spec, head_spec, col_spec, col_spec, row_shard_spec),
                         out_specs=(row_spec, row_spec, P('dp', None, 'tp', None, None), P('dp', 'tp', None, None), P('dp', None, 'tp'), P('dp', None, 'tp'), P('dp', 'tp', None), P('dp', None), P('dp', None)),
                         check_vma=False)
```
